256 devices in a mesh: req: 2 (over y), seq: 64 (over z, x), head: 2 (over core).
Axes of the slice: x: 4, y: 2, z: 16, core: 2. Of those that a mesh axis runs over, the one named last changes fastest.
The devices are a block of a 4x16x16 slice.
Arguments:
- cache_keys: bfloat16 [64, 4, 16384, 128], P('req', 'head', 'seq'), parts along dimension 0, may hold values from -6 to 6
- cache_values: bfloat16 [64, 4, 16384, 128], P('req', 'head', 'seq'), parts along dimension 0, may hold values from -6 to 6
- kept_mask: int32 [64, 4, 128], P('req', 'head', 'seq'), parts along dimension 0, may hold values from 0 to 1, as said below
- queries: bfloat16 [2, 64, 2048, 128], P('head', 'seq', 'req'), parts along dimension 2, may hold values from -64 to 64
- window_keys: bfloat16 [2, 64, 512, 128], P('head', 'seq', 'req'), parts along dimension 2, may hold values from -6 to 6
- window_values: bfloat16 [2, 64, 512, 128], P('head', 'seq', 'req'), parts along dimension 2, may hold values from -6 to 6
Outputs:
- kept_keys: bfloat16 [2, 64, 16384, 128], P('head', 'seq', 'req'), parts along dimension 2
- kept_values: bfloat16 [2, 64, 16384, 128], P('head', 'seq', 'req'), parts along dimension 2
- window_out: bfloat16 [2, 64, 2048, 128], P('head', 'seq', 'req'), parts along dimension 2
The draws below stay inside these ranges and needn't reach their ends.
There are 2 independent parts, one for each index of `req`. The reference program is written for one: setup_inputs(seed, part) draws one part's arguments, and reference() takes and returns one part's arrays. A program takes and returns all parts, laid end to end along the dimension named above; each array names one. Nothing has to cross between parts.
Inputs may be any that keep to these rules, and one draw needn't show every extreme that they name: `kept_mask`: for each layer l and KV head, each index of seq's 2 blocks hold at most 1 kept blocks, and layer l keeps exactly 1 * (S - (l * (S - max(1, S // 8))) // 31) blocks with S = 64, so layer 0 keeps 1 block on every index of seq.
All inputs are finite; a program needn't handle non-finite values.
Results may differ from the reference program's by a relative error of at most 0.0048.
Values may be sent and summed in bfloat16 or wider, within the bound.
No kernel may reach another device: no remote copies, remote signals or barrier semaphores. Data moves between devices by JAX's collectives and lax.ppermute only.
A program may use at most 128 MiB of HBM per device.

```python
import jax
import jax.numpy as jnp
from jax import lax

HEADS = 4
HD = 128
GROUP = 4
BLOCK = 128
WIN = 256
HPD = 2
LAYERS = 32
NTOK = 16384
NBLK = 128
BLK_DEV = 2
KEEP_MAX = 64
KEEP_TOK = 8192
N_HEAD = 2


def draw_kept_mask(key, part):
    shard_count = NBLK // BLK_DEV
    slot_cap = max(1, BLK_DEV // 2)
    fewest = max(1, shard_count // 8)
    first_key = jax.random.fold_in(key, 11)
    second_key = jax.random.fold_in(key, 12)
    shard_scores = jax.random.randint(first_key, (LAYERS, HEADS, shard_count), 0, 1 << 20) * shard_count + jnp.arange(shard_count, dtype=jnp.int32)
    shard_rank = jnp.argsort(jnp.argsort(shard_scores, axis=-1), axis=-1)
    layer_ids = jnp.arange(LAYERS, dtype=jnp.int32)
    chosen = shard_count - layer_ids * (shard_count - fewest) // (LAYERS - 1)
    shard_on = shard_rank < chosen[:, None, None]
    block_scores = jax.random.randint(second_key, (LAYERS, HEADS, shard_count, BLK_DEV), 0, 1 << 20) * BLK_DEV + jnp.arange(BLK_DEV, dtype=jnp.int32)
    block_rank = jnp.argsort(jnp.argsort(block_scores, axis=-1), axis=-1)
    block_on = block_rank < slot_cap
    return jnp.logical_and(shard_on[..., None], block_on).reshape(LAYERS, HEADS, NBLK).astype(jnp.int32)


def draw_queries(key, part):
    array_shape = (N_HEAD, LAYERS * HPD, GROUP * WIN, HD)
    first_key = jax.random.fold_in(key, 21)
    result = jnp.clip(jax.random.normal(first_key, array_shape, jnp.float32), -4.0, 4.0)
    return result.astype(jnp.bfloat16)


def block_levels(key, shape, pieces, low, largest):
    level, own = 1.0, jax.random.fold_in(key, 6)
    for dim, parts in pieces:
        draws = jnp.exp(jax.random.uniform(jax.random.fold_in(own, dim), (parts,), jnp.float32, low / len(pieces), largest / len(pieces)))
        level = level * jnp.repeat(draws, shape[dim] // parts).reshape([-1 if axis == dim else 1 for axis in range(len(shape))])
    return level


def normal_values(own_key, shape, width, reach, pieces=(), kind=jnp.bfloat16):
    values = width * jax.random.normal(own_key, shape, jnp.float32)
    if pieces:
        values = values * block_levels(own_key, shape, pieces, -0.22, 0.18)
    return jnp.clip(values, -reach, reach).astype(kind)


def setup_inputs(seed: int = 0, part: int = 0) -> dict:
    seeds = jax.random.split(jax.random.key(seed), 7)
    part_keys = jax.random.split(jax.random.fold_in(seeds[6], part), 7)
    cache_keys = normal_values(part_keys[0], (LAYERS, HEADS, NTOK, HD), 1.0, 6.0, ((1, 2), (2, 64)))
    cache_values = normal_values(part_keys[1], (LAYERS, HEADS, NTOK, HD), 1.0, 6.0, ((1, 2), (2, 64)))
    kept_mask = draw_kept_mask(jax.random.fold_in(jax.random.fold_in(seeds[6], part), 71), part)
    queries = draw_queries(jax.random.fold_in(jax.random.fold_in(seeds[6], part), 71), part)
    window_keys = normal_values(part_keys[4], (N_HEAD, LAYERS * HPD, WIN, HD), 1.0, 6.0, ((0, 2), (1, 64)))
    window_values = normal_values(part_keys[5], (N_HEAD, LAYERS * HPD, WIN, HD), 1.0, 6.0, ((0, 2), (1, 64)))
    return {"cache_keys": cache_keys, "cache_values": cache_values, "kept_mask": kept_mask, "queries": queries, "window_keys": window_keys, "window_values": window_values}


def attend(query_rows, positions, key_rows, value_rows, kept_len, live_len):
    scores = lax.dot_general(query_rows, key_rows, (((1,), (1,)), ((), ())), preferred_element_type=jnp.float32)
    scores = scores * (query_rows.shape[-1] ** -0.5)
    column = jnp.arange(key_rows.shape[0], dtype=jnp.int32)[None, :]
    is_live = jnp.where(column < kept_len, column < live_len, column - kept_len <= positions[:, None])
    scores = jnp.where(is_live, scores, -1e30)
    row_top = jnp.max(scores, axis=1, keepdims=True)
    weights = jnp.where(is_live, jnp.exp(scores - row_top), 0.0)
    row_total = jnp.sum(weights, axis=1, keepdims=True)
    blended = jnp.dot(weights.astype(jnp.bfloat16), value_rows, preferred_element_type=jnp.float32)
    return (blended / row_total).astype(jnp.bfloat16)


def reference(cache_keys, cache_values, kept_mask, queries, window_keys, window_values):
    head_share = HEADS // N_HEAD
    per_group = LAYERS * head_share
    owners = N_HEAD * per_group
    query_all = queries.reshape(owners, GROUP * WIN, HD)
    wkeys_all = window_keys.reshape(owners, WIN, HD)
    wvalues_all = window_values.reshape(owners, WIN, HD)
    positions = jnp.arange(GROUP * WIN, dtype=jnp.int32) % WIN
    slot_index = jnp.arange(KEEP_MAX, dtype=jnp.int32)

    def one_owner(owner_index):
        group_index = owner_index // per_group
        within = owner_index % per_group
        layer_index = within // head_share
        kv_head = group_index * head_share + within % head_share
        block_flags = kept_mask[layer_index, kv_head]
        kept_order = jnp.argsort(1 - block_flags, stable=True)[:KEEP_MAX]
        kept_count = jnp.sum(block_flags).astype(jnp.int32)
        is_kept = (slot_index < kept_count)[:, None]
        key_blocks = cache_keys[layer_index, kv_head].reshape(NBLK, BLOCK * HD)[kept_order]
        value_blocks = cache_values[layer_index, kv_head].reshape(NBLK, BLOCK * HD)[kept_order]
        kept_k = jnp.where(is_kept, key_blocks, jnp.zeros((), cache_keys.dtype)).reshape(KEEP_TOK, HD)
        kept_v = jnp.where(is_kept, value_blocks, jnp.zeros((), cache_values.dtype)).reshape(KEEP_TOK, HD)
        key_rows = jnp.concatenate([kept_k, wkeys_all[owner_index]], axis=0)
        value_rows = jnp.concatenate([kept_v, wvalues_all[owner_index]], axis=0)
        attended = attend(query_all[owner_index], positions, key_rows, value_rows, KEEP_TOK, kept_count * BLOCK)
        return kept_k, kept_v, attended

    kept_k, kept_v, attended = lax.map(one_owner, jnp.arange(owners, dtype=jnp.int32))
    return (kept_k.reshape(N_HEAD, per_group, KEEP_TOK, HD),
            kept_v.reshape(N_HEAD, per_group, KEEP_TOK, HD),
            attended.reshape(N_HEAD, per_group, GROUP * WIN, HD))
```

```python
import functools

import jax
import jax.numpy as jnp
from jax import lax
from jax.experimental import pallas as pl
from jax.experimental.pallas import tpu as pltpu
from jax.sharding import PartitionSpec as P


LANES = 4
FAR = 5
GROUPS = ((0, 4), (4, 6), (6, 8), (8, 10))
DEAD = -1e30
LOG2_E = 1.4426950408889634


VMEM = pl.BlockSpec(memory_space=pltpu.VMEM)
SMEM = pl.BlockSpec(memory_space=pltpu.SMEM)
ANY = pl.BlockSpec(memory_space=pl.ANY)


def place():
    index = lax.axis_index("seq")
    return index // LANES, index % LANES


def after(values, mark):
    return lax.optimization_barrier((values, mark))[0]


def pack_kernel(plan, planes, flags_ref, keys_ref, values_ref, *refs):
    outs, sems = refs[:-1], refs[-1]
    plane, lane = place()
    heads = flags_ref.shape[0]
    copies = []
    for out, slot, shift, hop in plan:
        owner = ((plane + (shift + planes)) % planes) * LANES + (lane + hop) % LANES
        block = owner * 2 + 1 - flags_ref[owner % heads, 0, owner // heads]
        for kind, source in enumerate((keys_ref, values_ref)):
            copies.append(
                pltpu.make_async_copy(source.at[block], outs[out].at[kind, slot], sems.at[len(copies)])
            )
            copies[-1].start()
    for copy in copies:
        copy.wait()


def pack(flags, keys, values, planes, plan, shapes):
    block = keys.shape[1:]
    return pl.pallas_call(
        functools.partial(pack_kernel, plan, planes),
        out_shape=[jax.ShapeDtypeStruct((2, count, *block), keys.dtype) for count in shapes],
        in_specs=[SMEM, ANY, ANY],
        out_specs=[VMEM] * len(shapes),
        scratch_shapes=[pltpu.SemaphoreType.DMA((2 * len(plan),))],
        cost_estimate=pl.CostEstimate(flops=1 << 20, bytes_accessed=sum(shapes) << 18, transcendentals=0),
    )(flags, keys, values)


def regroup_kernel(plan, count_in, *refs):
    for source, source_slot, out, out_slot in plan:
        refs[count_in + out][:, out_slot] = refs[source][:, source_slot]


def regroup(arrays, plan, shapes):
    block = arrays[0].shape[2:]
    return pl.pallas_call(
        functools.partial(regroup_kernel, plan, len(arrays)),
        out_shape=[jax.ShapeDtypeStruct((2, count, *block), arrays[0].dtype) for count in shapes],
        in_specs=[VMEM] * len(arrays),
        out_specs=[VMEM] * len(shapes),
        cost_estimate=pl.CostEstimate(flops=1 << 20, bytes_accessed=sum(shapes) << 18, transcendentals=0),
    )(*arrays)


def targets_kernel(live_ref, target_ref):
    shards = live_ref.shape[0]
    count = lax.fori_loop(0, shards, lambda i, total: total + live_ref[i], 0)

    def one(i, before):
        live = live_ref[i]
        target_ref[i] = jnp.where(live > 0, before, count + i - before)
        return before + live

    lax.fori_loop(0, shards, one, 0)


def targets_of(live):
    return pl.pallas_call(
        targets_kernel,
        out_shape=jax.ShapeDtypeStruct(live.shape, jnp.int32),
        in_specs=[SMEM],
        out_specs=SMEM,
        cost_estimate=pl.CostEstimate(flops=1 << 20, bytes_accessed=1 << 10, transcendentals=0),
        name="tables",
    )(live)


def blocks_of(query, key, scale, width):
    dots = lax.dot_general(query, key, (((1,), (1,)), ((), ())), preferred_element_type=jnp.float32)
    return [dots[:, at : at + width] * scale for at in range(0, key.shape[0], width)]


def largest(blocks, so_far=None):
    top = functools.reduce(jnp.maximum, blocks)
    top = jnp.broadcast_to(jnp.max(top, axis=1, keepdims=True), top.shape)
    return top if so_far is None else jnp.maximum(top, so_far)


def weigh(blocks, top, value):
    weights = [jnp.exp2(block - top) for block in blocks]
    rounded = jnp.concatenate([block.astype(value.dtype) for block in weights], axis=1)
    return sum(weights), jnp.dot(rounded, value, preferred_element_type=jnp.float32)


def attend_kernel(plan, planes, first, last, scale, *refs):
    refs = list(refs)
    live_ref, target_ref, query_ref = refs[:3]
    del refs[:3]
    if first:
        window_key_ref, window_value_ref, zero_ref = refs[:3]
        del refs[:3]
    else:
        zero_ref, _, _, top_in, total_in, blend_in = refs[:6]
        del refs[:6]
    pieces = refs[: len(plan)]
    del refs[: len(plan)]
    if last:
        kept_key_ref, kept_value_ref, out_ref, sems = refs
    else:
        kept_key_ref, kept_value_ref, top_ref, total_ref, blend_ref, sems = refs
    plane, lane = place()
    copies, lives = [], []
    for piece, blocks in zip(pieces, plan, strict=True):
        lives.append([])
        for slot, (shift, hop) in enumerate(blocks):
            source = ((plane + (planes - shift)) % planes) * LANES + (lane + (LANES - hop)) % LANES
            target, live = target_ref[source], live_ref[source]
            lives[-1].append(live)
            for kind, kept in enumerate((kept_key_ref, kept_value_ref)):
                copy = pltpu.make_async_copy(piece.at[kind, slot], kept.at[target], sems.at[len(copies)])
                blank = pltpu.make_async_copy(zero_ref, kept.at[target], sems.at[len(copies)])
                pl.when(live > 0)(copy.start)
                pl.when(live == 0)(blank.start)
                copies.append(copy)
    block_len, width = zero_ref.shape
    rows = query_ref.shape[0]
    if first:
        tile = window_key_ref.shape[0]
    else:
        tile = rows // 4

    def one_tile(index, _):
        at = pl.ds(pl.multiple_of(index * tile, tile), tile)
        query = query_ref[at, :]
        if first:
            scores = blocks_of(query, window_key_ref[...], scale, width)
            row = lax.broadcasted_iota(jnp.int32, (tile, width), 0)
            column = lax.broadcasted_iota(jnp.int32, (tile, width), 1)
            scores = [jnp.where(column + i * width <= row, block, DEAD) for i, block in enumerate(scores)]
            top = largest(scores)
            total, blend = weigh(scores, top, window_value_ref[...])
        else:
            top, total, blend = top_in[at, :], total_in[at, :], blend_in[at, :]
        for pair in range(0, len(pieces), 2):
            scores = []
            for piece, flags in zip(pieces[pair : pair + 2], lives[pair : pair + 2], strict=True):
                key = piece[0].reshape(piece.shape[1] * block_len, width)
                for block, live in zip(blocks_of(query, key, scale, block_len), flags, strict=True):
                    scores.append(block + jnp.where(live > 0, 0.0, DEAD))
            new_top = largest(scores, top)
            fade = jnp.exp2(top - new_top)
            total, blend, top = total * fade, blend * fade, new_top
            value = [piece[1].reshape(piece.shape[1] * block_len, width) for piece in pieces[pair : pair + 2]]
            add_total, add_blend = weigh(scores, top, jnp.concatenate(value, axis=0))
            total, blend = total + add_total, blend + add_blend
        if last:
            out_ref[at, :] = (blend / jnp.sum(total, axis=1, keepdims=True)).astype(out_ref.dtype)
        else:
            top_ref[at, :], total_ref[at, :], blend_ref[at, :] = top, total, blend
        return 0

    lax.fori_loop(0, rows // tile, one_tile, 0)
    for copy in copies:
        copy.wait()


def attend(live, target, query, zero, pieces, plan, planes, window=None, state=None, last=False):
    first = state is None
    rows, width = query.shape
    blocks = sum(len(piece) for piece in plan)
    keep = live.shape[0]
    kept = jax.ShapeDtypeStruct((keep, *zero.shape), query.dtype)
    partial = jax.ShapeDtypeStruct((rows, width), jnp.float32)
    if first:
        operands = [live, target, query, *window, zero, *pieces]
        in_specs = [SMEM, SMEM] + [VMEM] * (4 + len(pieces))
        aliases = {}
    else:
        operands = [live, target, query, zero, *state, *pieces]
        in_specs = [SMEM, SMEM, VMEM, VMEM, ANY, ANY] + [VMEM] * (3 + len(pieces))
        aliases = {4: 0, 5: 1}
    outs = [kept, kept]
    out_specs = [ANY, ANY]
    if last:
        outs.append(jax.ShapeDtypeStruct((rows, width), query.dtype))
        out_specs.append(VMEM)
    else:
        outs += [partial] * 3
        out_specs += [VMEM] * 3
    scale = width ** (-0.5) * LOG2_E
    return pl.pallas_call(
        functools.partial(attend_kernel, plan, planes, first, last, scale),
        out_shape=outs,
        in_specs=in_specs,
        out_specs=out_specs,
        scratch_shapes=[pltpu.SemaphoreType.DMA((2 * blocks,))],
        input_output_aliases=aliases,
        compiler_params=pltpu.CompilerParams(vmem_limit_bytes=16 << 20),
        cost_estimate=pl.CostEstimate(
            flops=4 * rows * width * blocks * zero.shape[0],
            bytes_accessed=blocks << 17,
            transcendentals=rows * blocks * zero.shape[0],
        ),
    )(*operands)


def step(cache_keys, cache_values, kept_mask, queries, window_keys, window_values):
    layer_count, head_share, token_count, width = cache_keys.shape
    blocks_here = kept_mask.shape[2]
    block_len = token_count // blocks_here
    shards = lax.axis_size("seq")
    planes = shards // LANES
    owners = layer_count * head_share
    assert blocks_here == 2 and owners == shards and shards % LANES == 0

    def send(array, shift, hop):
        pairs = []
        for index in range(shards):
            plane, lane = divmod(index, LANES)
            pairs.append((index, (plane + shift) % planes * LANES + (lane + hop) % LANES))
        return lax.ppermute(array, "seq", pairs)

    shifts = sorted((s - planes // 2 + 1 for s in range(planes)), key=lambda s: (-abs(s), -s))
    far, near = shifts[:FAR], shifts[FAR:-1]
    hops = range(LANES)
    keys = cache_keys.reshape(owners * 2, block_len, width)
    values = cache_values.reshape(owners * 2, block_len, width)
    flags = kept_mask.transpose(1, 2, 0)

    plan = [(i, hop, shift, hop) for i, shift in enumerate((*far, 0)) for hop in hops]
    *far_out, own_out = pack(flags, keys, values, planes, plan, [LANES] * (FAR + 1))
    far_in = [send(array, shift, 0) for array, shift in zip(far_out, far, strict=True)]
    plan = [(hop, i, shift, hop) for hop in hops for i, shift in enumerate(near)]
    near_out = pack(after(flags, own_out), keys, values, planes, plan, [len(near)] * LANES)
    near_lane = [near_out[0]] + [send(near_out[hop], 0, hop) for hop in hops[1:]]
    plan = [(hop, i, i, hop) for i in range(len(near)) for hop in hops]
    near_mid = regroup(near_lane, plan, [LANES] * len(near))
    near_in = [send(array, shift, 0) for array, shift in zip(near_mid, near, strict=True)]

    has_block = after(jnp.max(kept_mask, axis=2).reshape(owners, 1), near_mid[0])
    live = lax.all_to_all(has_block, "seq", split_axis=0, concat_axis=0, tiled=True).reshape(shards)
    target = targets_of(live)

    far_in = after(far_in, target)
    plan = [(i, hop, hop, i) for i in range(FAR + 1) for hop in hops]
    far_mid = regroup([*far_in, own_out], plan, [FAR + 1] * LANES)
    far_end = [far_mid[0]] + [send(far_mid[hop], 0, hop) for hop in hops[1:]]

    query = queries[0, 0]
    zero = jnp.zeros((block_len, width), query.dtype)
    plan = [[(shift, hop) for shift in (*far, 0)] for hop in hops]
    state = attend(live, target, query, zero, far_end, plan, planes, window=(window_keys[0, 0], window_values[0, 0]))
    plan = [[(shift, hop) for hop in hops] for shift in near]
    for first, end in GROUPS:
        *state, = attend(
            live, target, query, zero, near_in[first:end], plan[first:end], planes, state=state,
            last=end == len(near),
        )
    kept_k, kept_v, out = state
    return (
        kept_k.reshape(1, 1, shards * block_len, width),
        kept_v.reshape(1, 1, shards * block_len, width),
        out[None, None],
    )


def solution(mesh):
    in_specs = (
        P("req", "head", "seq", None),
        P("req", "head", "seq", None),
        P("req", "head", "seq"),
        P("head", "seq", "req", None),
        P("head", "seq", "req", None),
        P("head", "seq", "req", None),
    )
    out_specs = (
        P("head", "seq", "req", None),
        P("head", "seq", "req", None),
        P("head", "seq", "req", None),
    )
    return jax.shard_map(step, mesh=mesh, in_specs=in_specs, out_specs=out_specs, check_vma=False)
```
